512 devices in a mesh: dp: 8 (over y_hi, x), expert: 64 (over z, y_lo, core).
Axes of the slice: x: 4, y: 8 (y_hi: 2, y_lo: 4; y = y_hi * 4 + y_lo), z: 8, core: 2. Of those that a mesh axis runs over, the one named last changes fastest.
Arguments:
- tokens: bfloat16 [65536, 1024], P(('dp', 'expert')), may hold values from -6 to 6
- out_grad: bfloat16 [65536, 1024], P(('dp', 'expert')), may hold values from -6 to 6
- expert_ids: int32 [65536, 3], P(('dp', 'expert')), may hold values from 0 to 63, all different within a row; in each aligned block of 128 rows (0 to 127, 128 to 255, ...) at most 7 rows name the same one
- gate_probs: float32 [65536, 3], P(('dp', 'expert')), may hold values from 0.1 to 0.6
- saved_pre: bfloat16 [8, 64, 448, 1536], P('dp', 'expert'), may hold values from -6 to 6
- gate_weight: bfloat16 [64, 1024, 768], P('expert', 'dp'), may hold values from -0.1875 to 0.1875
- up_weight: bfloat16 [64, 1024, 768], P('expert', 'dp'), may hold values from -0.1875 to 0.1875
- down_weight: bfloat16 [64, 1024, 768], P('expert', 'dp'), may hold values from -0.21875 to 0.21875
- basis: bfloat16 [64, 1024, 256], P('expert', 'dp'), may hold values from -0.1875 to 0.1875
Outputs:
- in_grad: bfloat16 [65536, 1024], P(('dp', 'expert'))
- proj_grads: float32 [64, 3, 256, 768], P('expert', None, 'dp')
The draws below stay inside these ranges and needn't reach their ends.
Inputs may be any that keep to these rules, and one draw needn't show every extreme that they name: `expert_ids`: each token names 3 different experts. The rows of one device name one expert at most 7 times, and on some devices some expert exactly 7 times.
All inputs are finite; a program needn't handle non-finite values.
Results may differ from the reference program's by a relative error of at most 0.0091.
Values may be sent and summed in bfloat16 or wider, within the bound.
A program may use at most 64 MiB of HBM per device.

```python
import math
import jax
import jax.numpy as jnp
import numpy as np
from jax import lax

D = 1024
FF = 768
RANK = 256
TOPK = 3
TOK_DEV = 128
EXPERTS = 64
CAP = 7
SLOTS = 448
TOKENS = 65536
N_DP = 8
N_EXPERT = 64


def block_scale(stream_key, extent, cuts, smallest, largest):
    loudness, own = 1.0, jax.random.fold_in(stream_key, 6)
    for dim, blocks in cuts:
        draws = jnp.exp(jax.random.uniform(jax.random.fold_in(own, dim), (blocks,), jnp.float32, smallest / len(cuts), largest / len(cuts)))
        loudness = loudness * jnp.repeat(draws, extent[dim] // blocks).reshape([-1 if axis == dim else 1 for axis in range(len(extent))])
    return loudness


def assign_block(own_key, own, number, rows, amount, top, reach, slope):
    order = jax.random.permutation(own_key, amount)
    packed, ordinary = load_shares(amount, rows * top, reach, slope, True), load_shares(amount, rows * top, reach, slope, False)
    places = jnp.arange(amount)

    def named(sizes, rotation):
        used = int((sizes > 0).sum())
        fixed = max(1, used // 4)
        moved = fixed + (places - fixed + rotation * (used - fixed)) % max(1, amount - fixed)
        return jnp.zeros((amount,), jnp.int32).at[order[jnp.where(places < fixed, places, moved)]].set(jnp.asarray(sizes, jnp.int32))

    sizes = jnp.where(number % 4 == 0, named(packed, number // 4), named(ordinary, number - number // 4 - 1))
    mixed = jax.random.permutation(jax.random.fold_in(own, 3), amount)
    source_of, sink = mixed[0:amount // 2 * 2:2], mixed[1:amount // 2 * 2:2]
    margin = jnp.minimum(sizes[source_of] - 1, reach - sizes[sink]) // 2
    margin = jnp.where((source_of == order[0]) | (sink == order[0]) | (sizes[sink] == 0), 0, jnp.maximum(margin, 0))
    moved = jax.random.randint(jax.random.fold_in(own, 4), (amount // 2,), 0, 1 << 20) % (margin + 1)
    sizes = sizes.at[source_of].add(-moved).at[sink].add(moved)
    members = jnp.searchsorted(jnp.cumsum(sizes), jnp.arange(rows * top), side="right").astype(jnp.int32)
    grid = members.reshape(top, rows).T
    grid = grid[jax.random.permutation(jax.random.fold_in(own, 1), rows)]
    rotation = jax.random.randint(jax.random.fold_in(own, 2), (rows, 1), 0, top)
    return jnp.take_along_axis(grid, (jnp.arange(top)[None, :] + rotation) % top, axis=1)


def load_shares(count, total, limit, skew, full):
    portions = [(1 << 20) // math.isqrt(grade ** skew) + 1 for grade in range(1, count + 1)]
    largest = limit if full else min(limit, max(-(-total // count), total * portions[0] // sum(portions)))
    least = 1 if total - largest >= count - 1 else 0
    counts, surplus = [largest] + [least] * (count - 1), total - largest - least * (count - 1)
    while surplus > 0:
        candidates = [i for i in range(1, count) if counts[i] < largest] or [i for i in range(1, count) if counts[i] < limit]
        mass, budget = sum([portions[i] for i in candidates]), surplus
        for i in candidates:
            addition = min(limit - counts[i], max(1, budget * portions[i] // mass), surplus)
            counts[i] = counts[i] + addition
            surplus = surplus - addition
    return np.array(counts)


def scatter_about(rng, dims, width, reach, shards=(), kind=jnp.bfloat16):
    entries = width * jax.random.normal(rng, dims, jnp.float32)
    if shards:
        entries = entries * block_scale(rng, dims, shards, -0.22, 0.18)
    return jnp.clip(entries, -reach, reach).astype(kind)


def setup_inputs(seed: int = 0) -> dict:
    arg_keys = jax.random.split(jax.random.key(seed), 10)
    tokens = scatter_about(arg_keys[0], (TOKENS, D), 1.0, 6.0, ((0, 512),))
    out_grad = scatter_about(arg_keys[1], (TOKENS, D), 1.0, 6.0, ((0, 512),))
    expert_ids_keys = jax.random.split(jax.random.fold_in(arg_keys[2], 1), TOKENS // TOK_DEV)
    expert_ids_turns = jax.random.permutation(jax.random.fold_in(arg_keys[2], 3), TOKENS // TOK_DEV)
    expert_ids = jax.vmap(lambda own, number: assign_block(jax.random.fold_in(arg_keys[2], 2), own, number, TOK_DEV, EXPERTS, TOPK, CAP, 2))(expert_ids_keys, expert_ids_turns).reshape((TOKENS, TOPK))
    gate_probs = jnp.clip(0.1 + 0.5 * jax.random.uniform(arg_keys[3], (TOKENS, TOPK), jnp.float32) ** block_scale(arg_keys[3], (TOKENS, TOPK), ((0, 512),), -0.2, 0.2), 0.1, 0.6)
    saved_pre = scatter_about(arg_keys[4], (N_DP, EXPERTS, SLOTS, 2 * FF), 1.5, 6.0, ((0, 8), (1, 64)))
    gate_weight = scatter_about(arg_keys[5], (EXPERTS, D, FF), D ** -0.5, 0.1875, ((0, 64), (1, 8)))
    up_weight = scatter_about(arg_keys[6], (EXPERTS, D, FF), D ** -0.5, 0.1875, ((0, 64), (1, 8)))
    down_weight = scatter_about(arg_keys[7], (EXPERTS, D, FF), FF ** -0.5, 0.21875, ((0, 64), (1, 8)))
    basis = scatter_about(arg_keys[8], (EXPERTS, D, RANK), D ** -0.5, 0.1875, ((0, 64), (1, 8)))
    return {"tokens": tokens, "out_grad": out_grad, "expert_ids": expert_ids, "gate_probs": gate_probs, "saved_pre": saved_pre, "gate_weight": gate_weight, "up_weight": up_weight, "down_weight": down_weight, "basis": basis}


def slot_tables(expert_ids):
    devices = N_DP * N_EXPERT
    ids = expert_ids.reshape(devices, TOK_DEV, TOPK)
    onehot = (ids[:, :, :, None] == jnp.arange(EXPERTS, dtype=jnp.int32)[None, None, None, :]).astype(jnp.int32)
    per_token = jnp.sum(onehot, axis=2)
    before = jnp.cumsum(per_token, axis=1) - per_token
    position = jnp.sum(onehot * before[:, :, None, :], axis=3)
    device = jnp.arange(devices, dtype=jnp.int32)[:, None, None]
    group = device // N_EXPERT
    source = device % N_EXPERT
    flat = (group * EXPERTS + ids) * SLOTS + source * CAP + position
    token_index = device * TOK_DEV + jnp.arange(TOK_DEV, dtype=jnp.int32)[None, :, None]
    token_index = jnp.broadcast_to(token_index, ids.shape)
    choice_index = jnp.broadcast_to(jnp.arange(TOPK, dtype=jnp.int32)[None, None, :], ids.shape)
    table_token = jnp.full((N_DP * EXPERTS * SLOTS,), -1, jnp.int32).at[flat.reshape(-1)].set(token_index.reshape(-1))
    table_choice = jnp.zeros((N_DP * EXPERTS * SLOTS,), jnp.int32).at[flat.reshape(-1)].set(choice_index.reshape(-1))
    return table_token.reshape(N_DP, EXPERTS, SLOTS), table_choice.reshape(N_DP, EXPERTS, SLOTS)


def reference(tokens, out_grad, expert_ids, gate_probs, saved_pre, gate_weight, up_weight, down_weight, basis):
    table_token, table_choice = slot_tables(expert_ids)

    def per_expert(accum, expert):
        w_gate = gate_weight[expert]
        w_up = up_weight[expert]
        w_down = down_weight[expert]
        w_basis = basis[expert]

        def per_group(carry, group):
            total, projected = carry
            taken = table_token[group, expert]
            chosen = table_choice[group, expert]
            filled = taken >= 0
            picked = jnp.maximum(taken, 0).astype(jnp.int32)
            x_rows = jnp.where(filled[:, None], tokens[picked], jnp.zeros((), jnp.bfloat16))
            weight_pick = gate_probs[picked, chosen]
            scaled = (out_grad[picked].astype(jnp.float32) * weight_pick[:, None]).astype(jnp.bfloat16)
            dy_rows = jnp.where(filled[:, None], scaled, jnp.zeros((), jnp.bfloat16))
            pre = saved_pre[group, expert].astype(jnp.float32)
            gate_pre = pre[:, :FF]
            up_pre = pre[:, FF:]
            hidden_grad = jnp.dot(dy_rows, w_down, preferred_element_type=jnp.float32)
            x_proj = jnp.dot(x_rows, w_basis, preferred_element_type=jnp.float32).astype(jnp.bfloat16)
            dy_proj = jnp.dot(dy_rows, w_basis, preferred_element_type=jnp.float32).astype(jnp.bfloat16)
            sig = jax.nn.sigmoid(gate_pre)
            hid = (gate_pre * sig * up_pre).astype(jnp.bfloat16)
            up_grad = (hidden_grad * gate_pre * sig).astype(jnp.bfloat16)
            gate_grad = (hidden_grad * up_pre * sig * (1.0 + gate_pre * (1.0 - sig))).astype(jnp.bfloat16)
            terms = jnp.stack([
                jnp.dot(x_proj.T, gate_grad, preferred_element_type=jnp.float32),
                jnp.dot(x_proj.T, up_grad, preferred_element_type=jnp.float32),
                jnp.dot(dy_proj.T, hid, preferred_element_type=jnp.float32)])
            row_grad = jnp.dot(gate_grad, w_gate.T, preferred_element_type=jnp.float32)
            row_grad = row_grad + jnp.dot(up_grad, w_up.T, preferred_element_type=jnp.float32)
            row_grad = row_grad.astype(jnp.bfloat16).astype(jnp.float32)
            row_grad = jnp.where(filled[:, None], row_grad, jnp.zeros((), jnp.float32))
            total = total.at[picked].add(row_grad)
            return (total, projected + terms), None

        start = (accum, jnp.zeros((3, RANK, FF), jnp.float32))
        (accum, projected), unused = lax.scan(per_group, start, jnp.arange(N_DP, dtype=jnp.int32))
        return accum, projected

    accum = jnp.zeros((TOKENS, D), jnp.float32)
    accum, proj_grads = lax.scan(per_expert, accum, jnp.arange(EXPERTS, dtype=jnp.int32))
    return accum.astype(jnp.bfloat16), proj_grads
```

```python
import jax
import jax.numpy as jnp
from jax import lax
from jax.experimental import pallas as pl
from jax.experimental.pallas import tpu as pltpu
from jax.sharding import PartitionSpec as P

MESH = pl.DeviceIdType.MESH
F32 = jnp.float32
BF16 = jnp.bfloat16

N_X = 4
N_DP = 8
N_OWN = 64
CAP = 7
SLOTS = 448
TOK = 128
D = 1024
FF = 768
RANK = 256
LT = D // 128
PART = RANK // N_DP
BLK = 64
N_BLK = SLOTS // BLK


def iota(shape, dim):
    return lax.broadcasted_iota(jnp.int32, shape, dim)


def dot(a, b):
    return jnp.dot(a, b, preferred_element_type=F32)


def dot_t(a, b):
    return lax.dot_general(a, b, (((1,), (1,)), ((), ())), preferred_element_type=F32)


def t_dot(a, b):
    return lax.dot_general(a, b, (((0,), (0,)), ((), ())), preferred_element_type=F32)


def pack_rows(x, perm, buf, at):
    halves = []
    for h in range(2):
        part = x[32 * h : 32 * h + 32]
        halves.append(jnp.concatenate([part[:, 128 * j : 128 * j + 128] for j in range(LT)], axis=0))
    out = dot(perm, jnp.concatenate(halves, axis=1))
    for h in range(2):
        piece = out[:, 128 * h : 128 * h + 128].reshape(32, LT, 128).astype(BF16)
        buf[pl.ds(at + 32 * h, 32)] = piece


def unpack_rows(buf, at, perm_t):
    halves = [
        buf[pl.ds(at + 32 * h, 32)].astype(F32).reshape(32 * LT, 128).astype(BF16) for h in range(2)
    ]
    out = dot(perm_t, jnp.concatenate(halves, axis=1)).astype(BF16)
    rows = []
    for h in range(2):
        rows.append(
            jnp.concatenate(
                [out[32 * j : 32 * j + 32, 128 * h : 128 * h + 128] for j in range(LT)], axis=1
            )
        )
    return jnp.concatenate(rows, axis=0)


def wait_bytes(ref, sem):
    pltpu.make_async_copy(ref, ref, sem).wait()


def kernel(
    tok_ref, og_ref, ids_ref, probs_ref, pre_hbm, gate_ref, up_ref, down_ref, basis_ref,
    in_ref, proj_ref,
    pre_ref, full_d, full_g, full_u, full_b,
    pick_ref, wrow_ref, perm_ref, perm_t_ref,
    dy_send, dy_recv, x_send, x_recv, back_send, back_recv,
    dy_rows, x_rows, hg_ref, hid_ref, ug_ref, gg_ref, rows_ref,
    part_send, part_recv, cross_send, cross_recv,
    pre_sem, own_sem, w_send, y_sem, xa_sem, xb_sem,
    a_send, a_recv, a_own, r_send, r_recv,
):
    dp = lax.axis_index("dp")
    me = lax.axis_index("expert")
    hi, x = dp // N_X, lax.rem(dp, N_X)
    other = lax.rem(dp + N_X, N_DP)
    z, r = me // 8, lax.rem(me, 8)
    x_peers = [(hi * N_X + lax.rem(x + k, N_X), me) for k in (1, 3, 2)]
    partner = (other, me)

    def peer(k):
        return lax.rem(z + lax.rem(k, 8), 8) * 8 + lax.rem(r + k // 8, 8)

    barrier = pltpu.get_barrier_semaphore()
    for dev in x_peers + [partner]:
        pl.semaphore_signal(barrier, inc=1, device_id=dev, device_id_type=MESH)

    @pl.loop(1, N_OWN)
    def _(k):
        pl.semaphore_signal(barrier, inc=1, device_id=(dp, peer(k)), device_id_type=MESH)

    pre_copy = pltpu.make_async_copy(pre_hbm, pre_ref, pre_sem)
    pre_copy.start()
    pl.semaphore_wait(barrier, N_OWN + 3)

    mats = [(down_ref, full_d), (gate_ref, full_g), (up_ref, full_u), (basis_ref, full_b)]

    def remote(src, dst, send, recv, dev):
        pltpu.make_async_remote_copy(src, dst, send, recv, device_id=dev, device_id_type=MESH).start()

    for m, (own, full) in enumerate(mats):
        remote(own, full.at[dp], w_send.at[m], y_sem.at[m], partner)
    for m, (own, full) in enumerate(mats):
        for dev in x_peers:
            remote(own, full.at[dp], w_send.at[m], xa_sem.at[m], dev)
    for m, (own, full) in enumerate(mats):
        pltpu.make_async_copy(own, full.at[dp], own_sem.at[m]).start()

    o, i = iota((256, 256), 0), iota((256, 256), 1)
    perm_ref[...] = jnp.where(o == (i & 31) * 8 + (i >> 5), 1.0, 0.0).astype(BF16)
    perm_t_ref[...] = jnp.where(i == (o & 31) * 8 + (o >> 5), 1.0, 0.0).astype(BF16)
    experts = iota((N_OWN, TOK), 0)
    named = jnp.zeros((N_OWN, TOK), F32)
    weight = jnp.zeros((N_OWN, TOK), F32)
    for k in range(3):
        hit = jnp.broadcast_to(ids_ref[k : k + 1, :], (N_OWN, TOK)) == experts
        named = named + jnp.where(hit, 1.0, 0.0)
        weight = weight + jnp.where(hit, jnp.broadcast_to(probs_ref[k : k + 1, :], (N_OWN, TOK)), 0.0)
    earlier = jnp.where(iota((TOK, TOK), 0) < iota((TOK, TOK), 1), 1.0, 0.0).astype(BF16)
    before = dot(named.astype(BF16), earlier)
    rank = jnp.where(named > 0.0, before, -1.0).astype(BF16)
    rel = iota((SLOTS, N_OWN), 0) - CAP * iota((SLOTS, N_OWN), 1)
    spread = jnp.where((rel >= 0) & (rel < CAP), 1.0, 0.0)
    slot_rank = jnp.sum(spread * rel.astype(F32), axis=1, keepdims=True)
    at_rank = dot(spread.astype(BF16), rank)
    pick = jnp.where(at_rank == slot_rank, 1.0, 0.0)
    pick_ref[...] = pick.astype(BF16)
    weights = lax.dot_general(
        spread, weight, (((1,), (0,)), ((), ())),
        precision=lax.Precision.HIGHEST, preferred_element_type=F32,
    )
    wrow_ref[...] = jnp.broadcast_to(jnp.sum(pick * weights, axis=1, keepdims=True), (SLOTS, 128))

    def exchange(send, recv, n):
        @pl.loop(1, N_OWN)
        def _(k):
            d = peer(k)
            remote(
                send.at[pl.ds(d * CAP, CAP)], recv.at[pl.ds(me * CAP, CAP)],
                a_send.at[n], a_recv.at[n], (dp, d),
            )

        mine = pl.ds(me * CAP, CAP)
        pltpu.make_async_copy(send.at[mine], recv.at[mine], a_own.at[n]).start()

    def arrived(send, recv, n):
        mine = pl.ds(me * CAP, CAP)
        pltpu.make_async_copy(send.at[mine], recv.at[mine], a_own.at[n]).wait()
        wait_bytes(recv.at[pl.ds(0, SLOTS - CAP)], a_recv.at[n])

    @pl.loop(0, N_BLK)
    def _(b):
        at = pl.multiple_of(b * BLK, BLK)
        got = dot(pick_ref[pl.ds(at, BLK), :], og_ref[...])
        scale = wrow_ref[pl.ds(at, BLK), :]
        got = (got * jnp.concatenate([scale] * LT, axis=1)).astype(BF16)
        pack_rows(got, perm_ref[...], dy_send, at)

    exchange(dy_send, dy_recv, 0)

    @pl.loop(0, N_BLK)
    def _(b):
        at = pl.multiple_of(b * BLK, BLK)
        got = dot(pick_ref[pl.ds(at, BLK), :], tok_ref[...]).astype(BF16)
        pack_rows(got, perm_ref[...], x_send, at)

    for m, (own, full) in enumerate(mats):
        wait_bytes(full.at[0], y_sem.at[m])
        for dev in x_peers:
            remote(full.at[other], full.at[other], w_send.at[m], xb_sem.at[m], dev)

    exchange(x_send, x_recv, 1)

    def gathered(m):
        own, full = mats[m]
        pltpu.make_async_copy(own, full.at[dp], own_sem.at[m]).wait()
        wait_bytes(full.at[pl.ds(0, 3)], xa_sem.at[m])
        wait_bytes(full.at[pl.ds(0, 3)], xb_sem.at[m])

    arrived(dy_send, dy_recv, 0)

    @pl.loop(0, N_BLK)
    def _(b):
        at = pl.multiple_of(b * BLK, BLK)
        dy_rows[pl.ds(at, BLK), :] = unpack_rows(dy_recv, at, perm_t_ref[...])

    gathered(0)

    @pl.loop(0, FF // 256)
    def _(c):
        cols = pl.ds(pl.multiple_of(c * 256, 256), 256)
        hg_ref[:, cols] = dot(dy_rows[...], full_d[:, :, cols].reshape(D, 256))

    pre_copy.wait()

    @pl.loop(0, SLOTS // 16)
    def _(b):
        rows = pl.ds(pl.multiple_of(b * 16, 16), 16)
        g = pre_ref[rows, :FF].astype(F32)
        u = pre_ref[rows, FF:].astype(F32)
        h = hg_ref[rows, :]
        sig = jax.nn.sigmoid(g)
        gs = g * sig
        hid_ref[rows, :] = (gs * u).astype(BF16)
        ug_ref[rows, :] = (h * gs).astype(BF16)
        gg_ref[rows, :] = (h * u * sig * (1.0 + g * (1.0 - sig))).astype(BF16)

    gathered(1)
    gathered(2)

    @pl.loop(0, D // 256)
    def _(c):
        cols = pl.ds(pl.multiple_of(c * 256, 256), 256)
        two = pl.ds(c * 2, 2)
        total = dot_t(gg_ref[...], full_g[two].reshape(256, FF))
        total = total + dot_t(ug_ref[...], full_u[two].reshape(256, FF))
        rows_ref[:, cols] = total.astype(BF16)

    @pl.loop(0, N_BLK)
    def _(b):
        at = pl.multiple_of(b * BLK, BLK)
        pack_rows(rows_ref[pl.ds(at, BLK), :], perm_ref[...], back_send, at)

    exchange(back_send, back_recv, 2)

    gathered(3)
    basis = full_b[...].reshape(D, RANK)
    dy_proj = dot(dy_rows[...], basis).astype(BF16)

    def put(n, term):
        for q in range(N_DP):
            part_send[q % N_X, q // N_X, n] = term[PART * q : PART * (q + 1)].astype(BF16)

    put(2, t_dot(dy_proj, hid_ref[...]))
    arrived(x_send, x_recv, 1)

    @pl.loop(0, N_BLK)
    def _(b):
        at = pl.multiple_of(b * BLK, BLK)
        x_rows[pl.ds(at, BLK), :] = unpack_rows(x_recv, at, perm_t_ref[...])

    x_proj = dot(x_rows[...], basis).astype(BF16)
    put(0, t_dot(x_proj, gg_ref[...]))
    put(1, t_dot(x_proj, ug_ref[...]))

    for k, dev in enumerate(x_peers):
        to = lax.rem(x + (1, 3, 2)[k], N_X)
        remote(part_send.at[to], part_recv.at[k], r_send.at[0], r_recv.at[0], dev)
    wait_bytes(part_recv, r_recv.at[0])

    def sum_x(h):
        total = part_send[x, h].astype(F32)
        for k in range(3):
            total = total + part_recv[k, h].astype(F32)
        return total

    cross_send[...] = sum_x(1 - hi).astype(BF16)
    remote(cross_send, cross_recv, r_send.at[1], r_recv.at[1], partner)
    proj_ref[...] = sum_x(hi)

    arrived(back_send, back_recv, 2)

    @pl.loop(0, N_BLK)
    def _(b):
        at = pl.multiple_of(b * BLK, BLK)
        rows_ref[pl.ds(at, BLK), :] = unpack_rows(back_recv, at, perm_t_ref[...])

    in_ref[...] = t_dot(pick_ref[...], rows_ref[...]).astype(BF16)

    wait_bytes(cross_recv, r_recv.at[1])
    proj_ref[...] = proj_ref[...] + cross_recv[...].astype(F32)

    for m, (own, full) in enumerate(mats):
        wait_bytes(full.at[pl.ds(0, 7)], w_send.at[m])
    for n, buf in enumerate((dy_send, x_send, back_send)):
        wait_bytes(buf.at[pl.ds(0, SLOTS - CAP)], a_send.at[n])
    wait_bytes(part_recv, r_send.at[0])
    wait_bytes(cross_send, r_send.at[1])


def body(
    tokens, out_grad, expert_ids, gate_probs, saved_pre, gate_weight, up_weight, down_weight, basis
):
    vmem = pl.BlockSpec(memory_space=pltpu.VMEM)
    dma = pltpu.SemaphoreType.DMA
    packed = pltpu.VMEM((SLOTS, LT, 128), BF16)
    in_grad, proj = pl.pallas_call(
        kernel,
        out_shape=(
            jax.ShapeDtypeStruct((TOK, D), BF16),
            jax.ShapeDtypeStruct((3, PART, FF), F32),
        ),
        in_specs=[vmem] * 4 + [pl.BlockSpec(memory_space=pl.ANY)] + [vmem] * 4,
        out_specs=(vmem, vmem),
        scratch_shapes=[
            pltpu.VMEM((SLOTS, 2 * FF), BF16),
            pltpu.VMEM((N_DP, 128, FF), BF16),
            pltpu.VMEM((N_DP, 128, FF), BF16),
            pltpu.VMEM((N_DP, 128, FF), BF16),
            pltpu.VMEM((N_DP, 128, RANK), BF16),
            pltpu.VMEM((SLOTS, TOK), BF16),
            pltpu.VMEM((SLOTS, 128), F32),
            pltpu.VMEM((256, 256), BF16),
            pltpu.VMEM((256, 256), BF16),
            packed, packed, packed, packed, packed, packed,
            pltpu.VMEM((SLOTS, D), BF16),
            pltpu.VMEM((SLOTS, D), BF16),
            pltpu.VMEM((SLOTS, FF), F32),
            pltpu.VMEM((SLOTS, FF), BF16),
            pltpu.VMEM((SLOTS, FF), BF16),
            pltpu.VMEM((SLOTS, FF), BF16),
            pltpu.VMEM((SLOTS, D), BF16),
            pltpu.VMEM((N_X, 2, 3, PART, FF), BF16),
            pltpu.VMEM((3, 2, 3, PART, FF), BF16),
            pltpu.VMEM((3, PART, FF), BF16),
            pltpu.VMEM((3, PART, FF), BF16),
            dma, dma((4,)), dma((4,)), dma((4,)), dma((4,)), dma((4,)),
            dma((3,)), dma((3,)), dma((3,)), dma((2,)), dma((2,)),
        ],
        compiler_params=pltpu.CompilerParams(
            collective_id=0, has_side_effects=True, vmem_limit_bytes=48 << 20
        ),
    )(
        tokens, out_grad, expert_ids.T, gate_probs.T, saved_pre[0, 0],
        gate_weight[0], up_weight[0], down_weight[0], basis[0],
    )
    return in_grad, proj[None]


def solution(mesh):
    placed = (
        P(("dp", "expert"), None),
        P(("dp", "expert"), None),
        P(("dp", "expert"), None),
        P(("dp", "expert"), None),
        P("dp", "expert", None, None),
        P("expert", "dp", None),
        P("expert", "dp", None),
        P("expert", "dp", None),
        P("expert", "dp", None),
    )
    return jax.shard_map(
        body,
        mesh=mesh,
        in_specs=placed,
        out_specs=(P(("dp", "expert"), None), P("expert", None, "dp", None)),
        check_vma=False,
    )
```

```python
import jax
import jax.numpy as jnp
from jax import lax
from jax.experimental import pallas as pl
from jax.experimental.pallas import tpu as pltpu
from jax.sharding import PartitionSpec as P

MESH = pl.DeviceIdType.MESH
F32 = jnp.float32
BF16 = jnp.bfloat16

N_X = 4
N_DP = 8
N_OWN = 64
CAP = 7
SLOTS = 448
TOK = 128
D = 1024
FF = 768
RANK = 256
LT = D // 128
PART = RANK // N_DP
N_Y = 4
COL = SLOTS // N_Y


def iota(shape, dim):
    return lax.broadcasted_iota(jnp.int32, shape, dim)


def dot(a, b):
    return jnp.dot(a, b, preferred_element_type=F32)


def dot_t(a, b):
    return lax.dot_general(a, b, (((1,), (1,)), ((), ())), preferred_element_type=F32)


def t_dot(a, b):
    return lax.dot_general(a, b, (((0,), (0,)), ((), ())), preferred_element_type=F32)


def pack_rows(x, perm, buf, at):
    groups = []
    for g in range(COL // 16):
        part = x[16 * g : 16 * g + 16]
        groups.append(jnp.concatenate([part[:, 128 * j : 128 * j + 128] for j in range(LT)], axis=0))
    out = dot(perm, jnp.concatenate(groups, axis=1))
    for g in range(COL // 16):
        piece = out[:, 128 * g : 128 * g + 128].reshape(16, LT, 128).astype(BF16)
        buf[pl.ds(at + 16 * g, 16)] = piece


def unpack_rows(buf, at, perm_t):
    groups = [
        buf[pl.ds(at + 16 * g, 16)].astype(F32).reshape(16 * LT, 128).astype(BF16)
        for g in range(COL // 16)
    ]
    out = dot(perm_t, jnp.concatenate(groups, axis=1)).astype(BF16)
    rows = []
    for g in range(COL // 16):
        rows.append(
            jnp.concatenate(
                [out[16 * j : 16 * j + 16, 128 * g : 128 * g + 128] for j in range(LT)], axis=1
            )
        )
    return jnp.concatenate(rows, axis=0)


def wait_bytes(ref, sem):
    pltpu.make_async_copy(ref, ref, sem).wait()


def pick_slots(ids_ref, probs_ref, experts, earlier):
    n = experts.shape[0]
    named = jnp.zeros((n, TOK), F32)
    weight = jnp.zeros((n, TOK), F32)
    for k in range(3):
        hit = jnp.broadcast_to(ids_ref[k : k + 1, :], (n, TOK)) == experts
        named = named + jnp.where(hit, 1.0, 0.0)
        weight = weight + jnp.where(hit, jnp.broadcast_to(probs_ref[k : k + 1, :], (n, TOK)), 0.0)
    before = dot(named.astype(BF16), earlier)
    rank = jnp.where(named > 0.0, before, -1.0).astype(BF16)
    rel = iota((n * CAP, n), 0) - CAP * iota((n * CAP, n), 1)
    spread = jnp.where((rel >= 0) & (rel < CAP), 1.0, 0.0)
    slot_rank = jnp.sum(spread * rel.astype(F32), axis=1, keepdims=True)
    pick = jnp.where(dot(spread.astype(BF16), rank) == slot_rank, 1.0, 0.0)
    weights = lax.dot_general(
        spread, weight, (((1,), (0,)), ((), ())),
        precision=lax.Precision.HIGHEST, preferred_element_type=F32,
    )
    scale = jnp.broadcast_to(jnp.sum(pick * weights, axis=1, keepdims=True), (n * CAP, 128))
    return pick.astype(BF16), scale


def kernel(
    tok_hbm, og_hbm, ids_ref, probs_ref, pre_hbm, gate_hbm, up_hbm, down_hbm, basis_hbm,
    in_ref, proj_ref,
    tok_ref, og_ref, pre_ref, full_d, full_g, full_u, full_b,
    meta_ids, meta_probs, raw_ids, raw_probs, raw_tok, raw_og,
    pick_ref, col_pick, col_wrow, perm_ref, perm_t_ref,
    dy_send, dy_recv, x_send, x_recv, back_send, back_recv,
    dy_rows, x_rows, hg_ref, hid_ref, ug_ref, gg_ref, rows_ref,
    part_send, part_recv, cross_send, cross_recv,
    in_sem, own_sem, w_send, y_sem, x_sem,
    raw_send, raw_recv, a_send, a_recv, a_own, r_send, r_recv,
):
    dp = lax.axis_index("dp")
    me = lax.axis_index("expert")
    hi, x = dp // N_X, lax.rem(dp, N_X)
    other = lax.rem(dp + N_X, N_DP)
    z, r = me // 8, lax.rem(me, 8)
    core = lax.rem(r, 2)
    x_peers = [(hi * N_X + lax.rem(x + k, N_X), me) for k in (1, 3, 2)]
    right, left = x_peers[:2]
    partner = (other, me)

    def peer(k):
        return lax.rem(z + lax.rem(k, 8), 8), lax.rem(r + k // 8, 8)

    own_col = r // 2
    near_col = own_col + 1 - 2 * lax.rem(own_col, 2)
    far_cols = (lax.rem(own_col + 2, N_Y), lax.rem(near_col + 2, N_Y))
    cols = (own_col, near_col, *far_cols)
    near_dev = (dp, z * 8 + near_col * 2 + core)
    far_dev = (dp, z * 8 + far_cols[0] * 2 + core)

    def across(k):
        return lax.rem(z + lax.rem(3 * k + 4, 8), 8), lax.rem(lax.rem(r, 2) + k // 8, 2)

    def remote(src, dst, send, recv, dev):
        pltpu.make_async_remote_copy(src, dst, send, recv, device_id=dev, device_id_type=MESH).start()

    barrier = pltpu.get_barrier_semaphore()
    for dev in x_peers + [partner]:
        pl.semaphore_signal(barrier, inc=1, device_id=dev, device_id_type=MESH)

    @pl.loop(1, N_OWN)
    def _(k):
        to_z, to_r = peer(k)
        pl.semaphore_signal(barrier, inc=1, device_id=(dp, to_z * 8 + to_r), device_id_type=MESH)

    mats = [(down_hbm, full_d), (gate_hbm, full_g), (up_hbm, full_u), (basis_hbm, full_b)]
    own_copies = [pltpu.make_async_copy(own, full.at[dp], own_sem.at[m]) for m, (own, full) in enumerate(mats)]
    og_copy = pltpu.make_async_copy(og_hbm, og_ref, in_sem.at[0])
    tok_copy = pltpu.make_async_copy(tok_hbm, tok_ref, in_sem.at[1])
    pre_copy = pltpu.make_async_copy(pre_hbm, pre_ref, in_sem.at[2])
    for copy in [og_copy] + own_copies + [tok_copy, pre_copy]:
        copy.start()
    meta_ids[...] = jnp.zeros_like(meta_ids)
    meta_probs[...] = jnp.zeros_like(meta_probs)
    meta_ids[0:3, :] = ids_ref[...]
    meta_probs[0:3, :] = probs_ref[...]
    earlier = jnp.where(iota((TOK, TOK), 0) < iota((TOK, TOK), 1), 1.0, 0.0).astype(BF16)
    o, i = iota((128, 128), 0), iota((128, 128), 1)
    perm_ref[...] = jnp.where(o == (i & 15) * 8 + (i >> 4), 1.0, 0.0).astype(BF16)
    perm_t_ref[...] = jnp.where(i == (o & 15) * 8 + (o >> 4), 1.0, 0.0).astype(BF16)
    q = iota((N_OWN, TOK), 0)
    experts = ((q & 15) >> 1) * 8 + ((q >> 4) ^ own_col) * 2 + (q & 1)
    pick, scale = pick_slots(ids_ref, probs_ref, experts, earlier)
    pick_ref[...] = pick
    og_copy.wait()
    pl.semaphore_wait(barrier, N_OWN + 3)

    def cross_y(m):
        own, full = mats[m]
        remote(full.at[dp], full.at[dp], w_send.at[m], y_sem.at[m], partner)

    def to_sides(m, block, phase):
        full = mats[m][1]
        remote(full.at[block], full.at[block], w_send.at[m], x_sem.at[phase, 0, m], right)
        remote(full.at[block], full.at[block], w_send.at[m], x_sem.at[phase, 1, m], left)

    def pass_sides(m, phase):
        full = mats[m][1]
        row = (hi, 1 - hi)[phase] * N_X
        for side, frm, to in ((0, x + 3, right), (1, x + 1, left)):
            wait_bytes(full.at[0], x_sem.at[phase, side, m])
            piece = full.at[row + lax.rem(frm, N_X), pl.ds(64 * side, 64)]
            remote(piece, piece, w_send.at[m], x_sem.at[phase, 2, m], to)

    def pass_on(m):
        own, full = mats[m]
        wait_bytes(full.at[0], y_sem.at[m])
        to_sides(m, other, 1)

    def gathered(m):
        full = mats[m][1]
        wait_bytes(full.at[0], x_sem.at[0, 2, m])
        wait_bytes(full.at[0], x_sem.at[1, 2, m])

    def slots(index):
        return pl.ds(index * CAP, CAP)

    def send_slots(send, recv, n, j):
        slot = slots(z * 8 + cols[j] * 2 + core)

        @pl.loop(0, 16)
        def _(k):
            to_z, to_core = across(k)
            src, dst = send.at[slots(j * 16 + to_z * 2 + to_core)], recv.at[slot]

            @pl.when(k != 4)
            def _():
                remote(src, dst, a_send.at[n], a_recv.at[n], (dp, to_z * 8 + own_col * 2 + to_core))

        pltpu.make_async_copy(
            send.at[slots(j * 16 + z * 2 + core)], recv.at[slot], a_own.at[n]
        ).start()

    def arrived(recv, n, local):
        wait_bytes(recv.at[pl.ds(0, CAP * local)], a_own.at[n])
        wait_bytes(recv.at[pl.ds(0, SLOTS - CAP * local)], a_recv.at[n])

    def build(n, j, src, send):
        rows = pl.ds(j * COL, COL)
        got = dot(col_pick[rows, :], src[...])
        if n == 0:
            got = got * jnp.concatenate([col_wrow[rows, :]] * LT, axis=1)
        pack_rows(got.astype(BF16), perm_ref[...], send, j * COL)

    raws = (meta_ids, meta_probs, og_ref, tok_ref)
    others = (raw_ids, raw_probs, raw_og, raw_tok)

    def send_raw(n):
        remote(raws[n], others[n].at[1], raw_send.at[n], raw_recv.at[n, 1], far_dev)
        remote(raws[n], others[n].at[0], raw_send.at[n], raw_recv.at[n, 0], near_dev)

    def take_raw(n, j):
        wait_bytes(others[n].at[0], raw_recv.at[n, j - 1])
        if j == 2:
            remote(others[n].at[1], others[n].at[2], raw_send.at[n], raw_recv.at[n, 2], near_dev)

    def take_meta(j):
        take_raw(0, j)
        take_raw(1, j)
        pick, scale = pick_slots(raw_ids.at[j - 1], raw_probs.at[j - 1], experts[:16], earlier)
        col_pick[COL * j : COL * (j + 1)] = pick
        col_wrow[COL * j : COL * (j + 1)] = scale

    def deliver(n, j):
        src, send, recv = ((og_ref, dy_send, dy_recv), (tok_ref, x_send, x_recv))[n]
        if j:
            if n == 0:
                take_meta(j)
                take_raw(2, j)
            elif j != 2:
                take_raw(3, j)
            src = others[n + 2].at[j - 1]
        build(n, j, src, send)
        send_slots(send, recv, n, j)

    for n in range(3):
        send_raw(n)
    for copy in own_copies:
        copy.wait()
    for m in range(3):
        to_sides(m, dp, 0)
    cross_y(0)
    col_pick[0:COL] = pick_ref[0:COL]
    col_wrow[0:COL] = scale[0:COL]
    deliver(0, 0)
    pass_sides(0, 0)
    deliver(0, 1)
    deliver(0, 2)
    cross_y(1)
    tok_copy.wait()
    send_raw(3)
    pass_sides(1, 0)
    pass_sides(2, 0)
    pass_on(0)
    deliver(0, 3)
    deliver(1, 0)
    pass_sides(0, 1)
    pass_on(1)
    cross_y(2)
    cross_y(3)
    to_sides(3, dp, 0)
    take_raw(3, 2)
    arrived(dy_recv, 0, 4)

    @pl.loop(0, N_Y)
    def _(b):
        at = pl.multiple_of(b * COL, 16)
        dy_rows[pl.ds(at, COL), :] = unpack_rows(dy_recv, at, perm_t_ref[...])

    deliver(1, 1)
    deliver(1, 2)
    gathered(0)

    @pl.loop(0, FF // 256)
    def _(c):
        cols = pl.ds(pl.multiple_of(c * 256, 256), 256)
        hg_ref[:, cols] = dot(dy_rows[...], full_d[:, :, cols].reshape(D, 256))

    pass_sides(1, 1)
    pass_sides(3, 0)
    pre_copy.wait()

    @pl.loop(0, SLOTS // 16)
    def _(b):
        rows = pl.ds(pl.multiple_of(b * 16, 16), 16)
        g = pre_ref[rows, :FF].astype(F32)
        u = pre_ref[rows, FF:].astype(F32)
        h = hg_ref[rows, :]
        sig = jax.nn.sigmoid(g)
        gs = g * sig
        hid_ref[rows, :] = (gs * u).astype(BF16)
        ug_ref[rows, :] = (h * gs).astype(BF16)
        gg_ref[rows, :] = (h * u * sig * (1.0 + g * (1.0 - sig))).astype(BF16)

    pass_on(2)
    pass_on(3)
    deliver(1, 3)
    pass_sides(2, 1)
    pass_sides(3, 1)
    gathered(1)
    gathered(2)

    @pl.loop(0, D // 256)
    def _(c):
        cols = pl.ds(pl.multiple_of(c * 256, 256), 256)
        two = pl.ds(c * 2, 2)
        total = dot_t(gg_ref[...], full_g[two].reshape(256, FF))
        total = total + dot_t(ug_ref[...], full_u[two].reshape(256, FF))
        rows_ref[:, cols] = total.astype(BF16)

    @pl.loop(0, N_Y)
    def _(b):
        at = pl.multiple_of(b * COL, 16)
        pack_rows(rows_ref[pl.ds(at, COL), :], perm_ref[...], back_send, at)

    def place(to_r):
        col = to_r // 2
        apart = 2 * lax.rem(col // 2 + own_col // 2, 2) + lax.rem(col + own_col, 2)
        return slots(apart * 16 + z * 2 + core)

    def give_back(to_z, to_r):
        remote(
            back_send.at[slots(to_z * 8 + to_r)], back_recv.at[place(to_r)],
            a_send.at[2], a_recv.at[2], (dp, to_z * 8 + to_r),
        )

    @pl.loop(0, 16)
    def _(k):
        to_z, to_core = across(k)
        for col in (*far_cols, near_col):
            give_back(to_z, col * 2 + to_core)

        @pl.when(k != 4)
        def _():
            give_back(to_z, own_col * 2 + to_core)

    pltpu.make_async_copy(back_send.at[slots(me)], back_recv.at[place(r)], a_own.at[2]).start()

    gathered(3)
    basis = full_b[...].reshape(D, RANK)
    dy_proj = dot(dy_rows[...], basis).astype(BF16)

    def put(n, term):
        for p in range(N_DP):
            part_send[p % N_X, p // N_X, n] = term[PART * p : PART * (p + 1)].astype(BF16)

    put(2, t_dot(dy_proj, hid_ref[...]))
    arrived(x_recv, 1, 4)

    @pl.loop(0, N_Y)
    def _(b):
        at = pl.multiple_of(b * COL, 16)
        x_rows[pl.ds(at, COL), :] = unpack_rows(x_recv, at, perm_t_ref[...])

    x_proj = dot(x_rows[...], basis).astype(BF16)
    put(0, t_dot(x_proj, gg_ref[...]))
    put(1, t_dot(x_proj, ug_ref[...]))

    for k, dev in enumerate(x_peers):
        to = lax.rem(x + (1, 3, 2)[k], N_X)
        remote(part_send.at[to], part_recv.at[k], r_send.at[0], r_recv.at[0], dev)

    wait_bytes(part_recv, r_recv.at[0])

    def sum_x(h):
        total = part_send[x, h].astype(F32)
        for k in range(3):
            total = total + part_recv[k, h].astype(F32)
        return total

    cross_send[...] = sum_x(1 - hi).astype(BF16)
    remote(cross_send, cross_recv, r_send.at[1], r_recv.at[1], partner)
    proj_ref[...] = sum_x(hi)

    arrived(back_recv, 2, 1)

    @pl.loop(0, N_Y)
    def _(b):
        at = pl.multiple_of(b * COL, 16)
        rows_ref[pl.ds(at, COL), :] = unpack_rows(back_recv, at, perm_t_ref[...])

    in_ref[...] = t_dot(pick_ref[...], rows_ref[...]).astype(BF16)

    wait_bytes(cross_recv, r_recv.at[1])
    proj_ref[...] = proj_ref[...] + cross_recv[...].astype(F32)

    for m, (own, full) in enumerate(mats):
        wait_bytes(full.at[pl.ds(0, 7)], w_send.at[m])
    for n, dst in enumerate(others):
        wait_bytes(dst, raw_send.at[n])
    for n, buf, local in ((0, dy_send, 4), (1, x_send, 4), (2, back_send, 1)):
        wait_bytes(buf.at[pl.ds(0, SLOTS - CAP * local)], a_send.at[n])
    wait_bytes(part_recv, r_send.at[0])
    wait_bytes(cross_send, r_send.at[1])


def body(
    tokens, out_grad, expert_ids, gate_probs, saved_pre, gate_weight, up_weight, down_weight, basis
):
    vmem = pl.BlockSpec(memory_space=pltpu.VMEM)
    anywhere = pl.BlockSpec(memory_space=pl.ANY)
    dma = pltpu.SemaphoreType.DMA
    packed = pltpu.VMEM((SLOTS, LT, 128), BF16)
    in_grad, proj = pl.pallas_call(
        kernel,
        out_shape=(
            jax.ShapeDtypeStruct((TOK, D), BF16),
            jax.ShapeDtypeStruct((3, PART, FF), F32),
        ),
        in_specs=[anywhere] * 2 + [vmem] * 2 + [anywhere] * 5,
        out_specs=(vmem, vmem),
        scratch_shapes=[
            pltpu.VMEM((TOK, D), BF16),
            pltpu.VMEM((TOK, D), BF16),
            pltpu.VMEM((SLOTS, 2 * FF), BF16),
            pltpu.VMEM((N_DP, 128, FF), BF16),
            pltpu.VMEM((N_DP, 128, FF), BF16),
            pltpu.VMEM((N_DP, 128, FF), BF16),
            pltpu.VMEM((N_DP, 128, RANK), BF16),
            pltpu.VMEM((8, TOK), jnp.int32),
            pltpu.VMEM((8, TOK), F32),
            pltpu.VMEM((3, 8, TOK), jnp.int32),
            pltpu.VMEM((3, 8, TOK), F32),
            pltpu.VMEM((3, TOK, D), BF16),
            pltpu.VMEM((3, TOK, D), BF16),
            pltpu.VMEM((SLOTS, TOK), BF16),
            pltpu.VMEM((SLOTS, TOK), BF16),
            pltpu.VMEM((SLOTS, 128), F32),
            pltpu.VMEM((128, 128), BF16),
            pltpu.VMEM((128, 128), BF16),
            packed, packed, packed, packed, packed, packed,
            pltpu.VMEM((SLOTS, D), BF16),
            pltpu.VMEM((SLOTS, D), BF16),
            pltpu.VMEM((SLOTS, FF), F32),
            pltpu.VMEM((SLOTS, FF), BF16),
            pltpu.VMEM((SLOTS, FF), BF16),
            pltpu.VMEM((SLOTS, FF), BF16),
            pltpu.VMEM((SLOTS, D), BF16),
            pltpu.VMEM((N_X, 2, 3, PART, FF), BF16),
            pltpu.VMEM((3, 2, 3, PART, FF), BF16),
            pltpu.VMEM((3, PART, FF), BF16),
            pltpu.VMEM((3, PART, FF), BF16),
            dma((3,)), dma((4,)), dma((4,)), dma((4,)), dma((2, 3, 4)),
            dma((4,)), dma((4, 3)), dma((3,)), dma((3,)), dma((3,)), dma((2,)), dma((2,)),
        ],
        compiler_params=pltpu.CompilerParams(
            collective_id=0, has_side_effects=True, vmem_limit_bytes=67043328
        ),
    )(
        tokens, out_grad, expert_ids.T, gate_probs.T, saved_pre[0, 0],
        gate_weight[0], up_weight[0], down_weight[0], basis[0],
    )
    return in_grad, proj[None]


def solution(mesh):
    placed = (
        P(("dp", "expert"), None),
        P(("dp", "expert"), None),
        P(("dp", "expert"), None),
        P(("dp", "expert"), None),
        P("dp", "expert", None, None),
        P("expert", "dp", None),
        P("expert", "dp", None),
        P("expert", "dp", None),
        P("expert", "dp", None),
    )
    return jax.shard_map(
        body,
        mesh=mesh,
        in_specs=placed,
        out_specs=(P(("dp", "expert"), None), P("expert", None, "dp", None)),
        check_vma=False,
    )
```

```python
import jax
import jax.numpy as jnp
from jax import lax
from jax.experimental import pallas as pl
from jax.experimental.pallas import tpu as pltpu
from jax.sharding import PartitionSpec as P

MESH = pl.DeviceIdType.MESH
F32 = jnp.float32
BF16 = jnp.bfloat16

N_X = 4
N_DP = 8
N_OWN = 64
CAP = 7
SLOTS = 448
TOK = 128
D = 1024
FF = 768
RANK = 256
LT = D // 128
PART = RANK // N_DP
N_Y = 4
COL = SLOTS // N_Y


def iota(shape, dim):
    return lax.broadcasted_iota(jnp.int32, shape, dim)


def dot(a, b):
    return jnp.dot(a, b, preferred_element_type=F32)


def dot_t(a, b):
    return lax.dot_general(a, b, (((1,), (1,)), ((), ())), preferred_element_type=F32)


def t_dot(a, b):
    return lax.dot_general(a, b, (((0,), (0,)), ((), ())), preferred_element_type=F32)


def pack_rows(x, perm, buf, at):
    groups = []
    for g in range(COL // 16):
        part = x[16 * g : 16 * g + 16]
        groups.append(jnp.concatenate([part[:, 128 * j : 128 * j + 128] for j in range(LT)], axis=0))
    out = dot(perm, jnp.concatenate(groups, axis=1))
    for g in range(COL // 16):
        piece = out[:, 128 * g : 128 * g + 128].reshape(16, LT, 128).astype(BF16)
        buf[pl.ds(at + 16 * g, 16)] = piece


def unpack_rows(buf, at, perm_t):
    groups = [
        buf[pl.ds(at + 16 * g, 16)].astype(F32).reshape(16 * LT, 128).astype(BF16)
        for g in range(COL // 16)
    ]
    out = dot(perm_t, jnp.concatenate(groups, axis=1)).astype(BF16)
    rows = []
    for g in range(COL // 16):
        rows.append(
            jnp.concatenate(
                [out[16 * j : 16 * j + 16, 128 * g : 128 * g + 128] for j in range(LT)], axis=1
            )
        )
    return jnp.concatenate(rows, axis=0)


def wait_bytes(ref, sem):
    pltpu.make_async_copy(ref, ref, sem).wait()


def pick_slots(ids_ref, probs_ref, experts, earlier):
    n = experts.shape[0]
    named = jnp.zeros((n, TOK), F32)
    weight = jnp.zeros((n, TOK), F32)
    for k in range(3):
        hit = jnp.broadcast_to(ids_ref[k : k + 1, :], (n, TOK)) == experts
        named = named + jnp.where(hit, 1.0, 0.0)
        weight = weight + jnp.where(hit, jnp.broadcast_to(probs_ref[k : k + 1, :], (n, TOK)), 0.0)
    before = dot(named.astype(BF16), earlier)
    rank = jnp.where(named > 0.0, before, -1.0).astype(BF16)
    rel = iota((n * CAP, n), 0) - CAP * iota((n * CAP, n), 1)
    spread = jnp.where((rel >= 0) & (rel < CAP), 1.0, 0.0)
    slot_rank = jnp.sum(spread * rel.astype(F32), axis=1, keepdims=True)
    pick = jnp.where(dot(spread.astype(BF16), rank) == slot_rank, 1.0, 0.0)
    weights = lax.dot_general(
        spread, weight, (((1,), (0,)), ((), ())),
        precision=lax.Precision.HIGHEST, preferred_element_type=F32,
    )
    scale = jnp.broadcast_to(jnp.sum(pick * weights, axis=1, keepdims=True), (n * CAP, 128))
    return pick.astype(BF16), scale


def kernel(
    tok_hbm, og_hbm, ids_ref, probs_ref, pre_hbm, gate_hbm, up_hbm, down_hbm, basis_hbm,
    in_ref, proj_ref,
    tok_ref, og_ref, pre_ref, full_d, full_g, full_u, full_b,
    meta_ids, meta_probs, raw_ids, raw_probs, raw_tok, raw_og,
    pick_ref, col_pick, col_wrow, perm_ref, perm_t_ref,
    dy_send, dy_recv, x_send, x_recv, back_send, back_recv,
    dy_rows, x_rows, hg_ref, hid_ref, ug_ref, gg_ref, rows_ref,
    part_send, part_recv, cross_send, cross_recv,
    in_sem, own_sem, w_send, y_sem, x_sem,
    raw_send, raw_recv, a_send, a_recv, a_own, r_send, r_recv,
):
    dp = lax.axis_index("dp")
    me = lax.axis_index("expert")
    hi, x = dp // N_X, lax.rem(dp, N_X)
    other = lax.rem(dp + N_X, N_DP)
    z, r = me // 8, lax.rem(me, 8)
    core = lax.rem(r, 2)
    x_peers = [(hi * N_X + lax.rem(x + k, N_X), me) for k in (1, 3, 2)]
    right, left = x_peers[:2]
    partner = (other, me)

    def peer(k):
        return lax.rem(z + lax.rem(k, 8), 8), lax.rem(r + k // 8, 8)

    own_col = r // 2
    near_col = own_col + 1 - 2 * lax.rem(own_col, 2)
    far_cols = (lax.rem(own_col + 2, N_Y), lax.rem(near_col + 2, N_Y))
    cols = (own_col, near_col, *far_cols)
    near_dev = (dp, z * 8 + near_col * 2 + core)
    far_dev = (dp, z * 8 + far_cols[0] * 2 + core)

    def across(k):
        return lax.rem(z + lax.rem(3 * k + 4, 8), 8), lax.rem(lax.rem(r, 2) + k // 8, 2)

    def remote(src, dst, send, recv, dev):
        pltpu.make_async_remote_copy(src, dst, send, recv, device_id=dev, device_id_type=MESH).start()

    barrier = pltpu.get_barrier_semaphore()
    for dev in x_peers + [partner]:
        pl.semaphore_signal(barrier, inc=1, device_id=dev, device_id_type=MESH)

    @pl.loop(1, N_OWN)
    def _(k):
        to_z, to_r = peer(k)
        pl.semaphore_signal(barrier, inc=1, device_id=(dp, to_z * 8 + to_r), device_id_type=MESH)

    mats = [(down_hbm, full_d), (gate_hbm, full_g), (up_hbm, full_u), (basis_hbm, full_b)]
    own_copies = [pltpu.make_async_copy(own, full.at[dp], own_sem.at[m]) for m, (own, full) in enumerate(mats)]
    og_copy = pltpu.make_async_copy(og_hbm, og_ref, in_sem.at[0])
    tok_copy = pltpu.make_async_copy(tok_hbm, tok_ref, in_sem.at[1])
    pre_copy = pltpu.make_async_copy(pre_hbm, pre_ref, in_sem.at[2])
    for copy in [og_copy] + own_copies + [tok_copy, pre_copy]:
        copy.start()
    meta_ids[...] = jnp.zeros_like(meta_ids)
    meta_probs[...] = jnp.zeros_like(meta_probs)
    meta_ids[0:3, :] = ids_ref[...]
    meta_probs[0:3, :] = probs_ref[...]
    earlier = jnp.where(iota((TOK, TOK), 0) < iota((TOK, TOK), 1), 1.0, 0.0).astype(BF16)
    o, i = iota((128, 128), 0), iota((128, 128), 1)
    perm_ref[...] = jnp.where(o == (i & 15) * 8 + (i >> 4), 1.0, 0.0).astype(BF16)
    perm_t_ref[...] = jnp.where(i == (o & 15) * 8 + (o >> 4), 1.0, 0.0).astype(BF16)
    q = iota((N_OWN, TOK), 0)
    experts = ((q & 15) >> 1) * 8 + ((q >> 4) ^ own_col) * 2 + (q & 1)
    pick, scale = pick_slots(ids_ref, probs_ref, experts, earlier)
    pick_ref[...] = pick
    og_copy.wait()
    pl.semaphore_wait(barrier, N_OWN + 3)

    def cross_y(m):
        own, full = mats[m]
        remote(full.at[dp], full.at[dp], w_send.at[m], y_sem.at[m], partner)

    def to_sides(m, block, phase):
        full = mats[m][1]
        remote(full.at[block], full.at[block], w_send.at[m], x_sem.at[phase, 0, m], right)
        remote(full.at[block], full.at[block], w_send.at[m], x_sem.at[phase, 1, m], left)

    def pass_sides(m, phase):
        full = mats[m][1]
        row = (hi, 1 - hi)[phase] * N_X
        for side, frm, to in ((0, x + 3, right), (1, x + 1, left)):
            wait_bytes(full.at[0], x_sem.at[phase, side, m])
            piece = full.at[row + lax.rem(frm, N_X), pl.ds(64 * side, 64)]
            remote(piece, piece, w_send.at[m], x_sem.at[phase, 2, m], to)

    def pass_on(m):
        own, full = mats[m]
        wait_bytes(full.at[0], y_sem.at[m])
        to_sides(m, other, 1)

    def gathered(m):
        full = mats[m][1]
        wait_bytes(full.at[0], x_sem.at[0, 2, m])
        wait_bytes(full.at[0], x_sem.at[1, 2, m])

    def slots(index):
        return pl.ds(index * CAP, CAP)

    def send_slots(send, recv, n, j):
        slot = slots(z * 8 + cols[j] * 2 + core)

        @pl.loop(0, 16)
        def _(k):
            to_z, to_core = across(k)
            src, dst = send.at[slots(j * 16 + to_z * 2 + to_core)], recv.at[slot]

            @pl.when(k != 4)
            def _():
                remote(src, dst, a_send.at[n], a_recv.at[n], (dp, to_z * 8 + own_col * 2 + to_core))

        pltpu.make_async_copy(
            send.at[slots(j * 16 + z * 2 + core)], recv.at[slot], a_own.at[n]
        ).start()

    def arrived(recv, n, local):
        wait_bytes(recv.at[pl.ds(0, CAP * local)], a_own.at[n])
        wait_bytes(recv.at[pl.ds(0, SLOTS - CAP * local)], a_recv.at[n])

    def build(n, j, src, send):
        rows = pl.ds(j * COL, COL)
        got = dot(col_pick[rows, :], src[...])
        if n == 0:
            got = got * jnp.concatenate([col_wrow[rows, :]] * LT, axis=1)
        pack_rows(got.astype(BF16), perm_ref[...], send, j * COL)

    raws = (meta_ids, meta_probs, og_ref, tok_ref)
    others = (raw_ids, raw_probs, raw_og, raw_tok)

    def send_raw(n):
        remote(raws[n], others[n].at[1], raw_send.at[n], raw_recv.at[n, 1], far_dev)
        remote(raws[n], others[n].at[0], raw_send.at[n], raw_recv.at[n, 0], near_dev)

    def take_raw(n, j):
        wait_bytes(others[n].at[0], raw_recv.at[n, j - 1])
        if j == 2:
            remote(others[n].at[1], others[n].at[2], raw_send.at[n], raw_recv.at[n, 2], near_dev)

    def take_meta(j):
        take_raw(0, j)
        take_raw(1, j)
        pick, scale = pick_slots(raw_ids.at[j - 1], raw_probs.at[j - 1], experts[:16], earlier)
        col_pick[COL * j : COL * (j + 1)] = pick
        col_wrow[COL * j : COL * (j + 1)] = scale

    def deliver(n, j):
        src, send, recv = ((og_ref, dy_send, dy_recv), (tok_ref, x_send, x_recv))[n]
        if j:
            if n == 0:
                take_meta(j)
                take_raw(2, j)
            elif j != 2:
                take_raw(3, j)
            src = others[n + 2].at[j - 1]
        build(n, j, src, send)
        send_slots(send, recv, n, j)

    for n in range(3):
        send_raw(n)
    for copy in own_copies:
        copy.wait()
    for m in range(3):
        to_sides(m, dp, 0)
    cross_y(0)
    col_pick[0:COL] = pick_ref[0:COL]
    col_wrow[0:COL] = scale[0:COL]
    deliver(0, 0)
    pass_sides(0, 0)
    deliver(0, 1)
    deliver(0, 2)
    cross_y(1)
    tok_copy.wait()
    send_raw(3)
    pass_sides(1, 0)
    pass_sides(2, 0)
    deliver(0, 3)
    deliver(1, 0)
    pass_on(0)
    pass_sides(0, 1)
    cross_y(2)
    cross_y(3)
    to_sides(3, dp, 0)
    pass_on(1)
    take_raw(3, 2)
    arrived(dy_recv, 0, 4)

    @pl.loop(0, N_Y)
    def _(b):
        at = pl.multiple_of(b * COL, 16)
        dy_rows[pl.ds(at, COL), :] = unpack_rows(dy_recv, at, perm_t_ref[...])

    deliver(1, 1)
    deliver(1, 2)
    gathered(0)

    @pl.loop(0, FF // 256)
    def _(c):
        cols = pl.ds(pl.multiple_of(c * 256, 256), 256)
        hg_ref[:, cols] = dot(dy_rows[...], full_d[:, :, cols].reshape(D, 256))

    pass_sides(1, 1)
    pass_sides(3, 0)
    pre_copy.wait()

    @pl.loop(0, SLOTS // 16)
    def _(b):
        rows = pl.ds(pl.multiple_of(b * 16, 16), 16)
        g = pre_ref[rows, :FF].astype(F32)
        u = pre_ref[rows, FF:].astype(F32)
        h = hg_ref[rows, :]
        sig = jax.nn.sigmoid(g)
        gs = g * sig
        hid_ref[rows, :] = (gs * u).astype(BF16)
        ug_ref[rows, :] = (h * gs).astype(BF16)
        gg_ref[rows, :] = (h * u * sig * (1.0 + g * (1.0 - sig))).astype(BF16)

    pass_on(2)
    pass_on(3)
    deliver(1, 3)
    pass_sides(2, 1)
    pass_sides(3, 1)
    gathered(1)
    gathered(2)

    @pl.loop(0, D // 256)
    def _(c):
        cols = pl.ds(pl.multiple_of(c * 256, 256), 256)
        two = pl.ds(c * 2, 2)
        total = dot_t(gg_ref[...], full_g[two].reshape(256, FF))
        total = total + dot_t(ug_ref[...], full_u[two].reshape(256, FF))
        rows_ref[:, cols] = total.astype(BF16)

    @pl.loop(0, N_Y)
    def _(b):
        at = pl.multiple_of(b * COL, 16)
        pack_rows(rows_ref[pl.ds(at, COL), :], perm_ref[...], back_send, at)

    def place(to_r):
        col = to_r // 2
        apart = 2 * lax.rem(col // 2 + own_col // 2, 2) + lax.rem(col + own_col, 2)
        return slots(apart * 16 + z * 2 + core)

    def give_back(to_z, to_r):
        remote(
            back_send.at[slots(to_z * 8 + to_r)], back_recv.at[place(to_r)],
            a_send.at[2], a_recv.at[2], (dp, to_z * 8 + to_r),
        )

    @pl.loop(0, 16)
    def _(k):
        to_z, to_core = across(k)
        for col in (*far_cols, near_col):
            give_back(to_z, col * 2 + to_core)

        @pl.when(k != 4)
        def _():
            give_back(to_z, own_col * 2 + to_core)

    pltpu.make_async_copy(back_send.at[slots(me)], back_recv.at[place(r)], a_own.at[2]).start()

    gathered(3)
    basis = full_b[...].reshape(D, RANK)
    dy_proj = dot(dy_rows[...], basis).astype(BF16)

    def put(n, term):
        for p in range(N_DP):
            part_send[p % N_X, p // N_X, n] = term[PART * p : PART * (p + 1)].astype(BF16)

    put(2, t_dot(dy_proj, hid_ref[...]))
    arrived(x_recv, 1, 4)

    @pl.loop(0, N_Y)
    def _(b):
        at = pl.multiple_of(b * COL, 16)
        x_rows[pl.ds(at, COL), :] = unpack_rows(x_recv, at, perm_t_ref[...])

    x_proj = dot(x_rows[...], basis).astype(BF16)
    put(0, t_dot(x_proj, gg_ref[...]))
    put(1, t_dot(x_proj, ug_ref[...]))

    for k, dev in enumerate(x_peers):
        to = lax.rem(x + (1, 3, 2)[k], N_X)
        remote(part_send.at[to], part_recv.at[k], r_send.at[0], r_recv.at[0], dev)

    wait_bytes(part_recv, r_recv.at[0])

    def sum_x(h):
        total = part_send[x, h].astype(F32)
        for k in range(3):
            total = total + part_recv[k, h].astype(F32)
        return total

    cross_send[...] = sum_x(1 - hi).astype(BF16)
    remote(cross_send, cross_recv, r_send.at[1], r_recv.at[1], partner)
    proj_ref[...] = sum_x(hi)

    arrived(back_recv, 2, 1)

    @pl.loop(0, N_Y)
    def _(b):
        at = pl.multiple_of(b * COL, 16)
        rows_ref[pl.ds(at, COL), :] = unpack_rows(back_recv, at, perm_t_ref[...])

    in_ref[...] = t_dot(pick_ref[...], rows_ref[...]).astype(BF16)

    wait_bytes(cross_recv, r_recv.at[1])
    proj_ref[...] = proj_ref[...] + cross_recv[...].astype(F32)

    for m, (own, full) in enumerate(mats):
        wait_bytes(full.at[pl.ds(0, 7)], w_send.at[m])
    for n, dst in enumerate(others):
        wait_bytes(dst, raw_send.at[n])
    for n, buf, local in ((0, dy_send, 4), (1, x_send, 4), (2, back_send, 1)):
        wait_bytes(buf.at[pl.ds(0, SLOTS - CAP * local)], a_send.at[n])
    wait_bytes(part_recv, r_send.at[0])
    wait_bytes(cross_send, r_send.at[1])


def hand_out(a_hbm, b_hbm, a_out, b_out, a_ref, b_ref, sem):
    a_in = pltpu.make_async_copy(a_hbm, a_ref, sem.at[0])
    b_in = pltpu.make_async_copy(b_hbm, b_ref, sem.at[1])
    a_in.start()
    b_in.start()
    a_in.wait()
    a_back = pltpu.make_async_copy(a_ref, a_out, sem.at[2])
    a_back.start()
    b_in.wait()
    b_back = pltpu.make_async_copy(b_ref, b_out, sem.at[3])
    b_back.start()
    a_back.wait()
    b_back.wait()


def body(
    tokens, out_grad, expert_ids, gate_probs, saved_pre, gate_weight, up_weight, down_weight, basis
):
    vmem = pl.BlockSpec(memory_space=pltpu.VMEM)
    anywhere = pl.BlockSpec(memory_space=pl.ANY)
    dma = pltpu.SemaphoreType.DMA
    packed = pltpu.VMEM((SLOTS, LT, 128), BF16)
    in_grad, proj = pl.pallas_call(
        kernel,
        out_shape=(
            jax.ShapeDtypeStruct((TOK, D), BF16),
            jax.ShapeDtypeStruct((3, PART, FF), F32),
        ),
        in_specs=[anywhere] * 2 + [vmem] * 2 + [anywhere] * 5,
        out_specs=(vmem, vmem),
        scratch_shapes=[
            pltpu.VMEM((TOK, D), BF16),
            pltpu.VMEM((TOK, D), BF16),
            pltpu.VMEM((SLOTS, 2 * FF), BF16),
            pltpu.VMEM((N_DP, 128, FF), BF16),
            pltpu.VMEM((N_DP, 128, FF), BF16),
            pltpu.VMEM((N_DP, 128, FF), BF16),
            pltpu.VMEM((N_DP, 128, RANK), BF16),
            pltpu.VMEM((8, TOK), jnp.int32),
            pltpu.VMEM((8, TOK), F32),
            pltpu.VMEM((3, 8, TOK), jnp.int32),
            pltpu.VMEM((3, 8, TOK), F32),
            pltpu.VMEM((3, TOK, D), BF16),
            pltpu.VMEM((3, TOK, D), BF16),
            pltpu.VMEM((SLOTS, TOK), BF16),
            pltpu.VMEM((SLOTS, TOK), BF16),
            pltpu.VMEM((SLOTS, 128), F32),
            pltpu.VMEM((128, 128), BF16),
            pltpu.VMEM((128, 128), BF16),
            packed, packed, packed, packed, packed, packed,
            pltpu.VMEM((SLOTS, D), BF16),
            pltpu.VMEM((SLOTS, D), BF16),
            pltpu.VMEM((SLOTS, FF), F32),
            pltpu.VMEM((SLOTS, FF), BF16),
            pltpu.VMEM((SLOTS, FF), BF16),
            pltpu.VMEM((SLOTS, FF), BF16),
            pltpu.VMEM((SLOTS, D), BF16),
            pltpu.VMEM((N_X, 2, 3, PART, FF), BF16),
            pltpu.VMEM((3, 2, 3, PART, FF), BF16),
            pltpu.VMEM((3, PART, FF), BF16),
            pltpu.VMEM((3, PART, FF), BF16),
            dma((3,)), dma((4,)), dma((4,)), dma((4,)), dma((2, 3, 4)),
            dma((4,)), dma((4, 3)), dma((3,)), dma((3,)), dma((3,)), dma((2,)), dma((2,)),
        ],
        compiler_params=pltpu.CompilerParams(
            collective_id=0, has_side_effects=True, vmem_limit_bytes=67043328
        ),
    )(
        tokens, out_grad, expert_ids.T, gate_probs.T, saved_pre[0, 0],
        gate_weight[0], up_weight[0], down_weight[0], basis[0],
    )
    in_grad, proj = pl.pallas_call(
        hand_out,
        out_shape=(
            jax.ShapeDtypeStruct((TOK, D), BF16),
            jax.ShapeDtypeStruct((3, PART, FF), F32),
        ),
        in_specs=[anywhere, anywhere],
        out_specs=(anywhere, anywhere),
        scratch_shapes=[pltpu.VMEM((TOK, D), BF16), pltpu.VMEM((3, PART, FF), F32), dma((4,))],
        compiler_params=pltpu.CompilerParams(vmem_limit_bytes=67043328),
    )(in_grad, proj)
    return in_grad, proj[None]


def solution(mesh):
    placed = (
        P(("dp", "expert"), None),
        P(("dp", "expert"), None),
        P(("dp", "expert"), None),
        P(("dp", "expert"), None),
        P("dp", "expert", None, None),
        P("expert", "dp", None),
        P("expert", "dp", None),
        P("expert", "dp", None),
        P("expert", "dp", None),
    )
    return jax.shard_map(
        body,
        mesh=mesh,
        in_specs=placed,
        out_specs=(P(("dp", "expert"), None), P("expert", None, "dp", None)),
        check_vma=False,
    )
```
